32 devices in a mesh: mem: 4 (over z), state: 8 (over y, x, core).
Axes of the slice: x: 2, y: 2, z: 4, core: 2. Of those that a mesh axis runs over, the one named last changes fastest.
Arguments:
- anomalies: bfloat16 [64, 32, 32768], P('mem', None, 'state'), may hold values from -0.75 to 0.75
- alpha: bfloat16 [64, 32, 2048], P('mem', None, 'state'), may hold values from -6 to 6
- basis: bfloat16 [2048, 32768], P(None, 'state'), may hold values from -0.1875 to 0.1875
- gradient: bfloat16 [32, 32768], P(None, 'state'), may hold values from -6 to 6
- vertical_root: float32 [32, 32], replicated, may hold values from -1 to 1
- band_gain: float32 [16], replicated, may hold values from 0.25 to 2
- band: int32 [2048], P('state'), may hold values from 0 to 15
- order: int32 [64], replicated, may hold values from 0 to 63, each once
Outputs:
- increment: float32 [32, 32768], P(None, 'state')
- alpha_grad: float32 [64, 32, 2048], P('mem', None, 'state')
The draws below stay inside these ranges and needn't reach their ends.
Inputs may be any that keep to these rules, and one draw needn't show every extreme that they name: `order`: a permutation: every member is named by exactly one slot.
All inputs are finite; a program needn't handle non-finite values.
Results may differ from the reference program's by a relative error of at most 0.0029.
Values may be sent and summed in bfloat16 or wider, within the bound.
A program may use at most 128 MiB of HBM per device.

```python
import math
import jax
import jax.numpy as jnp
from jax import lax

LEVELS = 32
MODES = 2048
BANDS = 16
MEMBERS = 64
COLUMNS = 32768


def set_ends(result, key, least, top_value):
    spot = [jax.random.randint(jax.random.fold_in(key, axis), (), 0, length) for axis, length in enumerate(result.shape)]
    main_axis = result.shape.index(max(result.shape))
    neighbour = spot[:main_axis] + [(spot[main_axis] + 1) % result.shape[main_axis]] + spot[main_axis + 1:]
    return result.at[tuple(spot)].set(least).at[tuple(neighbour)].set(top_value)


def raised(values, key, source, target, blocks, factor):
    owner, partner = [(jnp.arange(values.shape[dim]) // (values.shape[dim] // blocks)).reshape([-1 if axis == dim else 1 for axis in range(values.ndim)]) for dim in (source, target)]
    chosen = jax.random.permutation(key, blocks)[partner]
    strong = (owner == chosen) | (owner == (partner + blocks // 2) % blocks)
    return jnp.where(strong, factor * values, values)


def steps_of(own_key, extent, shards, low, top_value):
    gain, own = 1.0, jax.random.fold_in(own_key, 6)
    for axis_at, parts in shards:
        heights = jnp.exp(jax.random.uniform(jax.random.fold_in(own, axis_at), (parts,), jnp.float32, low / len(shards), top_value / len(shards)))
        gain = gain * jnp.repeat(heights, extent[axis_at] // parts).reshape([-1 if axis == axis_at else 1 for axis in range(len(extent))])
    return gain


def normal_values(own_key, shape, spread, reach, cuts=(), kind=jnp.bfloat16):
    result = jax.random.normal(own_key, shape, jnp.float32) * spread
    if len(cuts) > 0:
        result = steps_of(own_key, shape, cuts, -0.22, 0.18) * result
    return jnp.clip(result, min=-reach, max=reach).astype(kind)


def noise_with(rng, dims, scale, most, pieces, heavy, kind=jnp.bfloat16):
    array = scale * jax.random.normal(rng, dims, jnp.float32)
    if pieces:
        array = array * steps_of(rng, dims, pieces, -0.22, 0.18)
    return jnp.clip(raised(array, jax.random.fold_in(rng, 3), *heavy), -most, most).astype(kind)


def setup_inputs(seed: int = 0) -> dict:
    arg_keys = jax.random.split(jax.random.key(seed), 9)
    return {
        "anomalies": normal_values(arg_keys[0], (MEMBERS, LEVELS, COLUMNS), 0.125, 0.75, ((0, 4), (2, 8))),
        "alpha": normal_values(arg_keys[1], (MEMBERS, LEVELS, MODES), 1.0, 6.0, ((0, 4), (2, 8))),
        "basis": noise_with(arg_keys[2], (MODES, COLUMNS), MODES ** -0.5, 0.1875, ((1, 8),), (1, 0, 8, 2.0)),
        "gradient": normal_values(arg_keys[3], (LEVELS, COLUMNS), 1.0, 6.0, ((1, 8),)),
        "vertical_root": normal_values(arg_keys[4], (LEVELS, LEVELS), LEVELS ** -0.5, 1.0, (), jnp.float32),
        "band_gain": jnp.clip(jnp.exp(jax.random.uniform(arg_keys[5], (BANDS,), jnp.float32, math.log(0.25), math.log(2.0))), 0.25, 2.0),
        "band": set_ends(jax.random.randint(arg_keys[6], (MODES,), 0, BANDS), jax.random.fold_in(arg_keys[6], 1), 0, BANDS - 1).astype(jnp.int32),
        "order": jax.random.permutation(arg_keys[7], MEMBERS).astype(jnp.int32),
    }


def reference(anomalies, alpha, basis, gradient, vertical_root, band_gain, band, order):
    high = lax.Precision.HIGHEST
    onehot = (band[:, None] == jnp.arange(BANDS, dtype=jnp.int32)[None, :]).astype(jnp.float32)
    filter_gain = jnp.sum(onehot * band_gain[None, :], axis=1)
    coef = jnp.einsum("ab,jbk->jak", vertical_root, alpha.astype(jnp.float32), precision=high)
    coef = (coef * filter_gain[None, None, :]).astype(jnp.bfloat16)
    inverse = jnp.zeros((MEMBERS,), jnp.int32).at[order].set(jnp.arange(MEMBERS, dtype=jnp.int32))
    member_coef = coef[inverse]
    grad_float = gradient.astype(jnp.float32)

    def one_member(running, member_items):
        member_anom, member_c = member_items
        member_field = jnp.dot(member_c, basis, preferred_element_type=jnp.float32)
        running = running + member_anom.astype(jnp.float32) * member_field
        weighted = (member_anom.astype(jnp.float32) * grad_float).astype(jnp.bfloat16)
        projected = lax.dot_general(weighted, basis, (((1,), (1,)), ((), ())), preferred_element_type=jnp.float32)
        return running, projected

    increment, projected = lax.scan(one_member, jnp.zeros((LEVELS, COLUMNS), jnp.float32), (anomalies, member_coef))
    slot_proj = projected[order]
    alpha_grad = jnp.einsum("ab,jak->jbk", vertical_root, slot_proj, precision=high) * filter_gain[None, None, :]
    return increment, alpha_grad
```

```python
import functools
import jax
import jax.numpy as jnp
from jax import lax
from jax.experimental import pallas as pl
from jax.experimental.pallas import tpu as pltpu
from jax.sharding import PartitionSpec as P

MESH = pl.DeviceIdType.MESH
F32 = jnp.float32
BF16 = jnp.bfloat16
NT = (((1,), (1,)), ((), ()))


def flip(a, k, n):
    out, bit = 0, 1
    while bit < n:
        out = out + lax.rem(lax.div(a, bit) + (k // bit) % 2, 2) * bit
        bit *= 2
    return out


def kernel(
    zn, sn, levels,
    table, gain, root, root_t, alpha, gradient, anomalies, basis,
    inc_out, grad_out,
    anom, base, weighted, coef_all, mine, pair_out, pair_in, rs_out, rs_in,
    pick_all, grad_all, acc, inc_own, inc_stage, inc_in, inc_red,
    anom_sem, base_sem, z_send, z_recv, pair_send, pair_recv, rs_send, rs_recv,
    pk_send, pk_recv, fw_send, fw_recv, g_send, g_recv, is_send, is_recv, ia_send, ia_recv,
):
    z = lax.axis_index("mem")
    s = lax.axis_index("state")
    chip, core = lax.div(s, 2), lax.rem(s, 2)
    qn = sn // 2
    partner = chip * 2 + (1 - core)
    rows, cols = alpha.shape
    columns = anom.shape[1]
    members = rows // levels
    high = lax.Precision.HIGHEST

    zpeer = [flip(z, k, zn) for k in range(zn)]
    qpeer = [flip(chip, k, qn) for k in range(qn)]

    def load_of(t, n):
        return pltpu.make_async_copy(basis.at[t], base.at[t], base_sem.at[n])

    order_of_q = list(range(qn - 1, -1, -1))
    anom_copy = pltpu.make_async_copy(anomalies, anom, anom_sem)
    anom_copy.start()
    loads = []
    for i, k in enumerate(order_of_q):
        loads.append((load_of(qpeer[k] * 2 + 1 - core, 2 * i), load_of(qpeer[k] * 2 + core, 2 * i + 1)))
        loads[-1][0].start()
        loads[-1][1].start()

    barrier = pltpu.get_barrier_semaphore()
    for k in range(1, zn):
        pl.semaphore_signal(barrier, inc=1, device_id={"mem": zpeer[k]}, device_id_type=MESH)
    for k in range(1, qn):
        pl.semaphore_signal(barrier, inc=1, device_id={"state": qpeer[k] * 2 + core}, device_id_type=MESH)
    pl.semaphore_signal(barrier, inc=1, device_id={"state": partner}, device_id_type=MESH)

    def to(src, dst, send, recv, **where):
        return pltpu.make_async_remote_copy(
            src_ref=src, dst_ref=dst, send_sem=send, recv_sem=recv, device_id=where, device_id_type=MESH
        )

    own_rows = pl.ds(z * members, members)
    coef = jnp.dot(root[...], alpha[...].astype(F32), precision=high, preferred_element_type=F32)
    coef_all[own_rows] = (coef * gain[...]).astype(BF16).reshape(members, levels, -1)
    pl.semaphore_wait(barrier, zn - 1 + qn)
    z_copies = [
        to(coef_all.at[own_rows], coef_all.at[own_rows], z_send.at[k], z_recv.at[k], mem=zpeer[k])
        for k in range(1, zn)
    ]
    for copy in z_copies:
        copy.start()

    anom_copy.wait()

    def weigh(m, carry):
        at = pl.ds(pl.multiple_of(m * levels, levels), levels)
        weighted[at, :] = (anom[at, :].astype(F32) * gradient[...].astype(F32)).astype(BF16)
        return carry

    lax.fori_loop(0, members, weigh, 0)

    pairs = [
        to(pair_out.at[i], pair_in.at[i], pair_send.at[i], pair_recv.at[i], state=partner) for i in range(qn)
    ]
    scatters = [
        to(rs_out.at[i], rs_in.at[i], rs_send.at[i], rs_recv.at[i], state=qpeer[k] * 2 + core)
        for i, k in enumerate(order_of_q[:-1])
    ]

    half = rows // 2

    def project(t, store):
        def part(h, carry):
            at = pl.ds(pl.multiple_of(h * half, half), half)
            store(at, lax.dot_general(weighted[at, :], base[t], NT, preferred_element_type=F32))
            return carry

        lax.fori_loop(0, 2, part, 0)

    def combine(i):
        pairs[i].wait_recv()
        total = mine[i] + pair_in[i]
        if i < qn - 1:
            rs_out[i] = total.astype(BF16)
            scatters[i].start()
        else:
            mine[i] = total

    for i, k in enumerate(order_of_q):
        loads[i][0].wait()

        def put_pair(at, v, i=i):
            pair_out[i, at, :] = v

        def put_mine(at, v, i=i):
            mine[i, at, :] = v

        project(qpeer[k] * 2 + 1 - core, put_pair)
        pairs[i].start()
        if i > 0:
            combine(i - 1)
        loads[i][1].wait()
        project(qpeer[k] * 2 + core, put_mine)

    for copy in z_copies:
        copy.wait_recv()
    for m in range(members):
        pick_all[s, pl.ds(m * levels, levels), :] = coef_all[table[0, m]]
    picks = [to(pick_all.at[s], pick_all.at[s], pk_send.at[0], pk_recv.at[0], state=partner)] + [
        to(pick_all.at[s], pick_all.at[s], pk_send.at[k], pk_recv.at[k], state=qpeer[k] * 2 + core)
        for k in range(1, qn)
    ]
    for copy in picks:
        copy.start()
    combine(qn - 1)

    pieces = zn
    width = columns // pieces

    def spread(t, first):
        def part(j, carry):
            at = pl.ds(pl.multiple_of(j * width, width), width)
            field = jnp.dot(pick_all[t], base[t, :, at], preferred_element_type=F32)
            acc[:, at] = field if first else acc[:, at] + field
            return carry

        lax.fori_loop(0, pieces, part, 0)

    spread(s, True)
    picks[0].wait_recv()
    spread(partner, False)

    for copy in scatters:
        copy.wait_recv()
    total = mine[qn - 1]
    for i in range(qn - 1):
        total = total + rs_in[i].astype(F32)
    grad = jnp.dot(root_t[...], total, precision=high, preferred_element_type=F32)
    grad_all[own_rows] = (grad * gain[...]).astype(BF16).reshape(members, levels, -1)
    g_copies = [
        to(grad_all.at[own_rows], grad_all.at[own_rows], g_send.at[k], g_recv.at[k], mem=zpeer[k])
        for k in range(1, zn)
    ]
    for copy in g_copies:
        copy.start()

    forwards = [None]
    for k in range(1, qn):
        t, o = qpeer[k] * 2 + core, qpeer[k] * 2 + 1 - core
        picks[k].wait_recv()
        forwards.append(to(pick_all.at[t], pick_all.at[t], fw_send.at[k], fw_recv.at[k], state=partner))
        forwards[k].start()
        spread(t, False)
        forwards[k].wait_recv()
        if k < qn - 1:
            spread(o, False)

    last = qpeer[qn - 1] * 2 + 1 - core
    sums = [None] + [
        to(inc_stage.at[k], inc_in.at[k], is_send.at[k], is_recv.at[k], mem=zpeer[k]) for k in range(1, zn)
    ]
    for k in list(range(1, zn)) + [0]:
        at = pl.ds(pl.multiple_of(zpeer[k] * width, width), width)

        def one(m, run, at=at):
            here = pl.ds(pl.multiple_of(m * 4 * levels, 4 * levels), 4 * levels)
            field = acc[here, at] + jnp.dot(pick_all[last, here, :], base[last, :, at], preferred_element_type=F32)
            prod = field * anom[here, at].astype(F32)
            for u in range(4):
                run = run + prod[u * levels : (u + 1) * levels]
            return run

        run = jnp.zeros((levels, width), F32)
        for m in range(members // 4):
            run = one(m, run)
        if k > 0:
            inc_stage[k] = run.astype(BF16)
            sums[k].start()
        else:
            inc_own[...] = run
    run = inc_own[...]
    for k in range(1, zn):
        sums[k].wait_recv()
        run = run + inc_in[k].astype(F32)
    inc_red[z] = run.astype(BF16)
    shares = [
        to(inc_red.at[z], inc_red.at[z], ia_send.at[k], ia_recv.at[k], mem=zpeer[k]) for k in range(1, zn)
    ]
    for copy in shares:
        copy.start()

    for copy in g_copies:
        copy.wait_recv()
    for m in range(members):
        grad_out[pl.ds(m * levels, levels), :] = grad_all[table[1, m]].astype(F32)

    for copy in shares:
        copy.wait_recv()
    for b in range(zn):
        inc_out[:, b * width : (b + 1) * width] = inc_red[b].astype(F32)
    for copy in z_copies + pairs + scatters + picks + forwards[1:] + g_copies + sums[1:] + shares:
        copy.wait_send()


def on_device(zn, sn, anomalies, alpha, basis, gradient, vertical_root, band_gain, band, order):
    z = lax.axis_index("mem")
    members, levels, columns = anomalies.shape
    mode_rows = alpha.shape[2]
    bands = band_gain.shape[0]
    rows = members * levels
    onehot = (band[:, None] == jnp.arange(bands, dtype=jnp.int32)[None, :]).astype(F32)
    gain = jnp.sum(onehot * band_gain[None, :], axis=1)[None, :]
    block = jnp.arange(rows, dtype=jnp.int32) // levels
    same = block[:, None] == block[None, :]
    root = jnp.where(same, jnp.tile(vertical_root, (members, members)), 0.0)
    root_t = jnp.where(same, jnp.tile(vertical_root.T, (members, members)), 0.0)
    here = z * members + jnp.arange(members, dtype=jnp.int32)
    slots = jnp.arange(order.shape[0], dtype=jnp.int32)
    slot_of = jnp.sum(jnp.where(order[None, :] == here[:, None], slots[None, :], 0), axis=1)
    member_of = jnp.sum(jnp.where(slots[None, :] == here[:, None], order[None, :], 0), axis=1)
    table = jnp.stack([slot_of, member_of])
    qn = sn // 2
    width = columns // zn
    vmem = pl.BlockSpec(memory_space=pltpu.VMEM)
    hbm = pl.BlockSpec(memory_space=pl.ANY)
    dma = pltpu.SemaphoreType.DMA
    increment, grads = pl.pallas_call(
        functools.partial(kernel, zn, sn, levels),
        out_shape=(
            jax.ShapeDtypeStruct((levels, columns), F32),
            jax.ShapeDtypeStruct((rows, mode_rows), F32),
        ),
        in_specs=[pl.BlockSpec(memory_space=pltpu.SMEM)] + [vmem] * 5 + [hbm] * 2,
        out_specs=(vmem, vmem),
        scratch_shapes=[
            pltpu.VMEM((rows, columns), BF16),
            pltpu.VMEM((sn, mode_rows, columns), BF16),
            pltpu.VMEM((rows, columns), BF16),
            pltpu.VMEM((zn * members, levels, mode_rows), BF16),
            pltpu.VMEM((qn, rows, mode_rows), F32),
            pltpu.VMEM((qn, rows, mode_rows), F32),
            pltpu.VMEM((qn, rows, mode_rows), F32),
            pltpu.VMEM((qn, rows, mode_rows), BF16),
            pltpu.VMEM((qn, rows, mode_rows), BF16),
            pltpu.VMEM((sn, rows, mode_rows), BF16),
            pltpu.VMEM((zn * members, levels, mode_rows), BF16),
            pltpu.VMEM((rows, columns), F32),
            pltpu.VMEM((levels, width), F32),
            pltpu.VMEM((zn, levels, width), BF16),
            pltpu.VMEM((zn, levels, width), BF16),
            pltpu.VMEM((zn, levels, width), BF16),
            dma, dma((sn,)), dma((zn,)), dma((zn,)), dma((qn,)), dma((qn,)), dma((qn,)), dma((qn,)),
            dma((qn,)), dma((qn,)), dma((qn,)), dma((qn,)), dma((zn,)), dma((zn,)), dma((zn,)), dma((zn,)),
            dma((zn,)), dma((zn,)),
        ],
        compiler_params=pltpu.CompilerParams(
            collective_id=0, has_side_effects=True, vmem_limit_bytes=58 * 2**20
        ),
    )(
        table, gain, root, root_t, alpha.reshape(rows, mode_rows), gradient,
        anomalies.reshape(rows, columns), basis.reshape(sn, mode_rows, columns),
    )
    return increment, grads.reshape(members, levels, mode_rows)


def solution(mesh):
    zn, sn = mesh.shape["mem"], mesh.shape["state"]
    return jax.shard_map(
        functools.partial(on_device, zn, sn),
        mesh=mesh,
        in_specs=(
            P("mem", None, "state"),
            P("mem", None, "state"),
            P(None, "state"),
            P(None, "state"),
            P(),
            P(),
            P("state"),
            P(),
        ),
        out_specs=(P(None, "state"), P("mem", None, "state")),
        check_vma=False,
    )
```

```python
import functools
import jax
import jax.numpy as jnp
from jax import lax
from jax.experimental import pallas as pl
from jax.experimental.pallas import tpu as pltpu
from jax.sharding import PartitionSpec as P

MESH = pl.DeviceIdType.MESH
F32 = jnp.float32
BF16 = jnp.bfloat16
NT = (((1,), (1,)), ((), ()))


def flip(a, k, n):
    out, bit = 0, 1
    while bit < n:
        out = out + lax.rem(lax.div(a, bit) + (k // bit) % 2, 2) * bit
        bit *= 2
    return out


def kernel(
    zn, sn, levels,
    table, gain, vroot, alpha, gradient, anomalies, basis,
    inc_out, grad_out,
    anom, base, weighted, coef_all, mine, pair_out, pair_in, rs_out, rs_in,
    pick_all, grad_all, acc, inc_own, inc_stage, inc_in, inc_red, pack, got,
    anom_sem, base_sem, z_send, z_recv, pair_send, pair_recv, rs_send, rs_recv,
    pk_send, pk_recv, fw_send, fw_recv, g_send, g_recv, is_send, is_recv, ia_send, ia_recv,
):
    z = lax.axis_index("mem")
    s = lax.axis_index("state")
    chip, core = lax.div(s, 2), lax.rem(s, 2)
    qn = sn // 2
    partner = chip * 2 + (1 - core)
    rows, cols = alpha.shape
    columns = anom.shape[1]
    members = rows // levels
    high = lax.Precision.HIGHEST

    zpeer = [flip(z, k, zn) for k in range(zn)]
    qpeer = [flip(chip, k, qn) for k in range(qn)]

    def load_of(t, n):
        return pltpu.make_async_copy(basis.at[t], base.at[t], base_sem.at[n])

    order_of_q = list(range(qn - 1, -1, -1))
    anom_copy = pltpu.make_async_copy(anomalies, anom, anom_sem)
    anom_copy.start()
    loads = []
    for i, k in enumerate(order_of_q):
        loads.append((load_of(qpeer[k] * 2 + 1 - core, 2 * i), load_of(qpeer[k] * 2 + core, 2 * i + 1)))
        loads[-1][0].start()
        loads[-1][1].start()

    barrier = pltpu.get_barrier_semaphore()
    for k in range(1, zn):
        pl.semaphore_signal(barrier, inc=1, device_id={"mem": zpeer[k]}, device_id_type=MESH)
    for k in range(1, qn):
        pl.semaphore_signal(barrier, inc=1, device_id={"state": qpeer[k] * 2 + core}, device_id_type=MESH)
    pl.semaphore_signal(barrier, inc=1, device_id={"state": partner}, device_id_type=MESH)

    def to(src, dst, send, recv, **where):
        return pltpu.make_async_remote_copy(
            src_ref=src, dst_ref=dst, send_sem=send, recv_sem=recv, device_id=where, device_id_type=MESH
        )

    own_rows = pl.ds(z * members, members)
    line = zn == 4
    outer = lax.div(lax.rem(z + 1, zn), 2) == 0
    inner = jnp.logical_not(outer)

    class Exchange:
        def __init__(self, row, held, mine, packed, send, recv):
            self.row, self.held, self.mine, self.packed = row, held, mine, packed
            own = held.at[own_rows]
            if not line:
                self.copies = [
                    to(own, own, send.at[k], recv.at[k], mem=zpeer[k]) for k in range(1, zn)
                ]
                return
            self.near = 1 + lax.rem(z, 2)
            self.far = lax.max(z - 1, 0) * 3 - lax.max(z - 2, 0) * 3
            rim = held.at[pl.ds(self.far * members, members)]
            kind = lax.rem(lax.div(z + 1, 2), 2)
            self.first = to(own, own, send.at[0], recv.at[kind], mem=self.near)
            self.from_rim = to(own, own, send.at[0], recv.at[0], mem=self.near)
            self.from_inner = to(own, own, send.at[0], recv.at[1], mem=self.near)
            self.relay = to(rim, rim, send.at[1], recv.at[2], mem=self.near)
            self.give = to(packed, mine, send.at[2], recv.at[3], mem=self.far)

        def start(self):
            for copy in [self.first] if line else self.copies:
                copy.start()

        def pass_on(self):
            if line:

                @pl.when(inner)
                def _():
                    self.from_rim.wait_recv()
                    self.relay.start()

        def pick(self, out, who):
            for m in range(members):
                out[pl.ds(m * levels, levels), :] = self.held[table[self.row, who * members + m]]

        def finish(self):
            if not line:
                for copy in self.copies:
                    copy.wait_recv()
                self.pick(self.mine, z)
                return

            @pl.when(inner)
            def _():
                self.from_inner.wait_recv()
                self.relay.wait_recv()
                self.pick(self.packed, self.far)
                self.give.start()
                self.pick(self.mine, z)

        def settle(self):
            if line:

                @pl.when(outer)
                def _():
                    self.give.wait_recv()

        def drain(self):
            if not line:
                for copy in self.copies:
                    copy.wait_send()
                return
            self.first.wait_send()

            @pl.when(inner)
            def _():
                self.relay.wait_send()
                self.give.wait_send()

    row_of = lax.broadcasted_iota(jnp.int32, (rows, levels), 0)
    level_of = lax.broadcasted_iota(jnp.int32, (rows, levels), 1)
    expand = jnp.where(lax.rem(row_of, levels) == level_of, 1.0, 0.0).astype(F32)
    here_of = lax.broadcasted_iota(jnp.int32, (rows, rows), 0)
    there_of = lax.broadcasted_iota(jnp.int32, (rows, rows), 1)
    same = lax.div(here_of, levels) == lax.div(there_of, levels)

    def blocks(tall):
        full = lax.dot_general(tall, expand, NT, precision=high, preferred_element_type=F32)
        return jnp.where(same, full, 0.0)

    root = blocks(jnp.dot(expand, vroot[...], precision=high, preferred_element_type=F32))
    coef = jnp.dot(root, alpha[...].astype(F32), precision=high, preferred_element_type=F32)
    coef_all[own_rows] = (coef * gain[...]).astype(BF16).reshape(members, levels, -1)
    pl.semaphore_wait(barrier, zn - 1 + qn)
    coef_ex = Exchange(0, coef_all, pick_all.at[s], pack.at[0], z_send, z_recv)
    coef_ex.start()

    anom_copy.wait()

    def weigh(m, carry):
        at = pl.ds(pl.multiple_of(m * levels, levels), levels)
        weighted[at, :] = (anom[at, :].astype(F32) * gradient[...].astype(F32)).astype(BF16)
        return carry

    lax.fori_loop(0, members, weigh, 0)

    pairs = [
        to(pair_out.at[i], pair_in.at[i], pair_send.at[i], pair_recv.at[i], state=partner) for i in range(qn)
    ]
    scatters = [
        to(rs_out.at[i], rs_in.at[i], rs_send.at[i], rs_recv.at[i], state=qpeer[k] * 2 + core)
        for i, k in enumerate(order_of_q[:-1])
    ]

    half = rows // 2

    def project(t, store):
        def part(h, carry):
            at = pl.ds(pl.multiple_of(h * half, half), half)
            store(at, lax.dot_general(weighted[at, :], base[t], NT, preferred_element_type=F32))
            return carry

        lax.fori_loop(0, 2, part, 0)

    def combine(i):
        pairs[i].wait_recv()
        total = mine[i] + pair_in[i]
        if i < qn - 1:
            rs_out[i] = total.astype(BF16)
            scatters[i].start()
        else:
            mine[i] = total

    for i, k in enumerate(order_of_q):
        loads[i][0].wait()

        def put_pair(at, v, i=i):
            pair_out[i, at, :] = v

        def put_mine(at, v, i=i):
            mine[i, at, :] = v

        project(qpeer[k] * 2 + 1 - core, put_pair)
        pairs[i].start()
        if i > 0:
            combine(i - 1)
        loads[i][1].wait()
        project(qpeer[k] * 2 + core, put_mine)
        if i == qn // 2 - 1:
            coef_ex.pass_on()

    coef_ex.finish()
    combine(qn - 1)
    coef_ex.settle()
    picks = [to(pick_all.at[s], pick_all.at[s], pk_send.at[0], pk_recv.at[0], state=partner)] + [
        to(pick_all.at[s], pick_all.at[s], pk_send.at[k], pk_recv.at[k], state=qpeer[k] * 2 + core)
        for k in range(1, qn)
    ]
    for copy in picks:
        copy.start()

    pieces = zn
    width = columns // pieces

    def spread(t, first):
        def part(j, carry):
            at = pl.ds(pl.multiple_of(j * width, width), width)
            field = jnp.dot(pick_all[t], base[t, :, at], preferred_element_type=F32)
            acc[:, at] = field if first else acc[:, at] + field
            return carry

        lax.fori_loop(0, pieces, part, 0)

    spread(s, True)
    for copy in scatters:
        copy.wait_recv()
    total = mine[qn - 1]
    for i in range(qn - 1):
        total = total + rs_in[i].astype(F32)
    root_t = blocks(lax.dot_general(expand, vroot[...], NT, precision=high, preferred_element_type=F32))
    grad = jnp.dot(root_t, total, precision=high, preferred_element_type=F32)
    grad_all[own_rows] = (grad * gain[...]).astype(BF16).reshape(members, levels, -1)
    grad_ex = Exchange(1, grad_all, got, pack.at[1], g_send, g_recv)
    grad_ex.start()
    picks[0].wait_recv()
    spread(partner, False)

    forwards = [None]
    for k in range(1, qn):
        t, o = qpeer[k] * 2 + core, qpeer[k] * 2 + 1 - core
        picks[k].wait_recv()
        forwards.append(to(pick_all.at[t], pick_all.at[t], fw_send.at[k], fw_recv.at[k], state=partner))
        forwards[k].start()
        spread(t, False)
        forwards[k].wait_recv()
        if k < qn - 1:
            spread(o, False)
        if k == qn // 2:
            grad_ex.pass_on()

    last = qpeer[qn - 1] * 2 + 1 - core
    sums = [None] + [
        to(inc_stage.at[k], inc_in.at[k], is_send.at[k], is_recv.at[k], mem=zpeer[k]) for k in range(1, zn)
    ]
    for k in list(range(1, zn)) + [0]:
        at = pl.ds(pl.multiple_of(zpeer[k] * width, width), width)

        def one(m, run, at=at):
            here = pl.ds(pl.multiple_of(m * 4 * levels, 4 * levels), 4 * levels)
            field = acc[here, at] + jnp.dot(pick_all[last, here, :], base[last, :, at], preferred_element_type=F32)
            prod = field * anom[here, at].astype(F32)
            for u in range(4):
                run = run + prod[u * levels : (u + 1) * levels]
            return run

        run = jnp.zeros((levels, width), F32)
        for m in range(members // 4):
            run = one(m, run)
        if k > 0:
            inc_stage[k] = run.astype(BF16)
            sums[k].start()
        else:
            inc_own[...] = run
    grad_ex.finish()
    run = inc_own[...]
    for k in range(1, zn):
        sums[k].wait_recv()
        run = run + inc_in[k].astype(F32)
    inc_red[z] = run.astype(BF16)
    shares = [
        to(inc_red.at[z], inc_red.at[z], ia_send.at[k], ia_recv.at[k], mem=zpeer[k]) for k in range(1, zn)
    ]
    for copy in shares:
        copy.start()

    grad_ex.settle()
    grad_out[...] = got[...]

    for copy in shares:
        copy.wait_recv()
    for b in range(zn):
        inc_out[:, b * width : (b + 1) * width] = inc_red[b]
    coef_ex.drain()
    grad_ex.drain()
    for copy in pairs + scatters + picks + forwards[1:] + sums[1:] + shares:
        copy.wait_send()


def on_device(zn, sn, anomalies, alpha, basis, gradient, vertical_root, band_gain, band, order):
    members, levels, columns = anomalies.shape
    mode_rows = alpha.shape[2]
    bands = band_gain.shape[0]
    rows = members * levels
    onehot = (band[:, None] == jnp.arange(bands, dtype=jnp.int32)[None, :]).astype(F32)
    gain = jnp.sum(onehot * band_gain[None, :], axis=1)[None, :]
    slots = jnp.arange(order.shape[0], dtype=jnp.int32)
    slot_of = jnp.sum(jnp.where(order[None, :] == slots[:, None], slots[None, :], 0), axis=1)
    table = jnp.stack([slot_of, order])
    qn = sn // 2
    width = columns // zn
    vmem = pl.BlockSpec(memory_space=pltpu.VMEM)
    hbm = pl.BlockSpec(memory_space=pl.ANY)
    dma = pltpu.SemaphoreType.DMA
    increment, grads = pl.pallas_call(
        functools.partial(kernel, zn, sn, levels),
        out_shape=(
            jax.ShapeDtypeStruct((levels, columns), BF16),
            jax.ShapeDtypeStruct((rows, mode_rows), BF16),
        ),
        in_specs=[pl.BlockSpec(memory_space=pltpu.SMEM)] + [vmem] * 4 + [hbm] * 2,
        out_specs=(vmem, vmem),
        scratch_shapes=[
            pltpu.VMEM((rows, columns), BF16),
            pltpu.VMEM((sn, mode_rows, columns), BF16),
            pltpu.VMEM((rows, columns), BF16),
            pltpu.VMEM((zn * members, levels, mode_rows), BF16),
            pltpu.VMEM((qn, rows, mode_rows), F32),
            pltpu.VMEM((qn, rows, mode_rows), F32),
            pltpu.VMEM((qn, rows, mode_rows), F32),
            pltpu.VMEM((qn, rows, mode_rows), BF16),
            pltpu.VMEM((qn, rows, mode_rows), BF16),
            pltpu.VMEM((sn, rows, mode_rows), BF16),
            pltpu.VMEM((zn * members, levels, mode_rows), BF16),
            pltpu.VMEM((rows, columns), F32),
            pltpu.VMEM((levels, width), F32),
            pltpu.VMEM((zn, levels, width), BF16),
            pltpu.VMEM((zn, levels, width), BF16),
            pltpu.VMEM((zn, levels, width), BF16),
            pltpu.VMEM((2, rows, mode_rows), BF16),
            pltpu.VMEM((rows, mode_rows), BF16),
            dma, dma((sn,)), dma((zn,)), dma((zn,)), dma((qn,)), dma((qn,)), dma((qn,)), dma((qn,)),
            dma((qn,)), dma((qn,)), dma((qn,)), dma((qn,)), dma((zn,)), dma((zn,)), dma((zn,)), dma((zn,)),
            dma((zn,)), dma((zn,)),
        ],
        compiler_params=pltpu.CompilerParams(
            collective_id=0, has_side_effects=True, vmem_limit_bytes=58 * 2**20
        ),
    )(
        table, gain, vertical_root, alpha.reshape(rows, mode_rows), gradient,
        anomalies.reshape(rows, columns), basis.reshape(sn, mode_rows, columns),
    )
    return increment.astype(F32), grads.astype(F32).reshape(members, levels, mode_rows)


def solution(mesh):
    zn, sn = mesh.shape["mem"], mesh.shape["state"]
    return jax.shard_map(
        functools.partial(on_device, zn, sn),
        mesh=mesh,
        in_specs=(
            P("mem", None, "state"),
            P("mem", None, "state"),
            P(None, "state"),
            P(None, "state"),
            P(),
            P(),
            P("state"),
            P(),
        ),
        out_specs=(P(None, "state"), P("mem", None, "state")),
        check_vma=False,
    )
```
